8 devices in a mesh: dp: 1 (over z), ri: 2 (over y), co: 2 (over x), ro: 2 (over core).
Axes of the slice: x: 2, y: 2, z: 1, core: 2. Of those that a mesh axis runs over, the one named last changes fastest.
Arguments:
- a_mat: bfloat16 [5120, 32768], P(('dp', 'ri', 'ro'), 'co')
- b_mat: bfloat16 [32768, 13824], P(('dp', 'ri', 'ro'), 'co')
Outputs:
- output: bfloat16 [5120, 13824], P(('dp', 'ri', 'ro'), 'co')
All inputs are finite; a program needn't handle non-finite values.
Results may differ from the reference program's by a relative error of at most 0.001.
Values are sent between devices in bfloat16 or wider.
A program may use at most 1 GiB of HBM per device.

```python
import jax
import jax.numpy as jnp

M_ROWS = 5120
N_COLS = 13824
K_DEPTH = 32768


def setup_inputs(seed: int = 0, part: int = 0) -> dict:
    base_key = jax.random.fold_in(jax.random.key(seed), part)
    key_a, key_b = jax.random.split(base_key)
    left_mat = jax.random.normal(key_a, (M_ROWS, K_DEPTH), jnp.float32)
    right_mat = jax.random.normal(key_b, (K_DEPTH, N_COLS), jnp.float32) * (K_DEPTH ** -0.5)
    return {"a_mat": left_mat.astype(jnp.bfloat16), "b_mat": right_mat.astype(jnp.bfloat16)}


def reference(a_mat, b_mat):
    product = jnp.dot(a_mat, b_mat, preferred_element_type=jnp.float32)
    return product.astype(jnp.bfloat16)
```

```python
import functools

import jax
import jax.numpy as jnp
from jax import lax
from jax.experimental import pallas as pl
from jax.experimental.pallas import tpu as pltpu
from jax.sharding import PartitionSpec as P

MESH = pl.DeviceIdType.MESH
PIECES = 16
EXTRA = 64


def _kernel(extra, tile, out_tile, a_ref, b_ref, c_ref, z_ref, x_ref, t_ref, bs_ref, ps_ref, pr_ref,
            acc, av, bv, prv, ov, zf_recv, zg_recv, t_recv, x_recv, b_recv, c_recv,
            y_send, f_send, x_send, b_send, c_send, a_sem, b_sem, p_sem, pr_sem, o_sem):
    ri, co, ro = lax.axis_index("ri"), lax.axis_index("co"), lax.axis_index("ro")
    diag = ri == co
    far = ri != co
    x_dev, y_dev, sib = {"co": 1 - co}, {"ri": 1 - ri}, {"ro": 1 - ro}

    half = a_ref.shape[0] // 2
    kt = a_ref.shape[1] // PIECES
    cols = b_ref.shape[1]
    own = PIECES // 2
    steps = 4 * PIECES
    f = jnp.where(diag, 0, half)
    g = half - f

    def kcols(j):
        return pl.ds(pl.multiple_of(lax.rem(j + own * ro, PIECES) * kt, kt), kt)

    def rows(base, n):
        return pl.ds(pl.multiple_of(base, 16), n)

    def remote(src, dst, send, recv, dev):
        return pltpu.make_async_remote_copy(src_ref=src, dst_ref=dst, send_sem=send, recv_sem=recv,
                                            device_id=dev, device_id_type=MESH)

    relay_rows = half + extra

    def first_y(j):
        return remote(a_ref.at[pl.ds(0, half), kcols(j)], z_ref.at[pl.ds(0, half), kcols(j)],
                      y_send, zf_recv.at[j], y_dev)

    def first_x(j):
        return remote(a_ref.at[pl.ds(half - extra, relay_rows), kcols(j)], t_ref.at[:, kcols(j)],
                      x_send, t_recv.at[j], x_dev)

    def relay(j):
        return remote(t_ref.at[:, kcols(j)], z_ref.at[pl.ds(half - extra, relay_rows), kcols(j)],
                      y_send, zf_recv.at[j], y_dev)

    def pass_diag(j):
        r = pl.ds(0, half - extra)
        return remote(z_ref.at[r, kcols(j)], z_ref.at[r, kcols(j)], f_send, zg_recv.at[j], x_dev)

    def pass_far(j):
        r = pl.ds(half, half)
        return remote(z_ref.at[r, kcols(j)], z_ref.at[r, kcols(j)], f_send, zg_recv.at[j], x_dev)

    def give_x(q):
        blk, j = q // PIECES, lax.rem(q, PIECES)
        at = (rows(blk * half, half), kcols(j))
        return remote(a_ref.at[at], x_ref.at[at], x_send, x_recv.at[q], x_dev)

    def give_b(i):
        r = rows(i * kt, kt)
        return remote(b_ref.at[r], bs_ref.at[r], b_send.at[i], b_recv.at[i], sib)

    def give_c(blk):
        r = rows(jnp.where(blk == 0, f, g), half)
        return remote(ps_ref.at[r], pr_ref.at[r], c_send.at[blk], c_recv.at[blk], y_dev)

    def base_of(blk):
        return jnp.where((blk == 0) | (blk == 3), f, g)

    def load_a(src, s):
        blk, j, slot = s // PIECES, lax.rem(s, PIECES), lax.rem(s, 2)
        return pltpu.make_async_copy(src.at[rows(base_of(blk), half), kcols(j)], av.at[slot], a_sem.at[slot])

    def load_b(src, i, s):
        slot = lax.rem(s, 2)
        return pltpu.make_async_copy(src.at[rows(i * kt, kt)], bv.at[slot], b_sem.at[slot])

    def start_b(s):
        blk, j = s // PIECES, lax.rem(s, PIECES)

        @pl.when(j < own)
        def _():
            load_b(b_ref, j, s).start()

        @pl.when(j >= own)
        def _():
            @pl.when(blk == 0)
            def _():
                give_b(j - own).wait_recv()
            load_b(bs_ref, j - own, s).start()

    barrier = pltpu.get_barrier_semaphore()
    for dev in (x_dev, y_dev, sib):
        pl.semaphore_signal(barrier, inc=1, device_id=dev, device_id_type=MESH)
    pl.semaphore_wait(barrier, 3)

    @pl.when(far)
    def _():
        def go(j, carry):
            first_x(j).start()
            first_y(j).start()
            return carry
        lax.fori_loop(0, PIECES, go, 0)

    @pl.when(diag)
    def _():
        give_x(0).start()
        give_x(1).start()

    def go_b(i, carry):
        give_b(i).start()
        return carry
    lax.fori_loop(0, own, go_b, 0)
    start_b(0)

    def step(s, carry):
        blk, j, slot = s // PIECES, lax.rem(s, PIECES), lax.rem(s, 2)

        @pl.when(s + 1 < steps)
        def _():
            start_b(s + 1)

        @pl.when(blk == 0)
        def _():
            @pl.when(diag)
            def _():
                first_y(j).wait_recv()
                pass_diag(j).start()
                load_a(z_ref, s).start()
                first_x(j).wait_recv()
                relay(j).start()

            @pl.when(far)
            def _():
                relay(j).wait_recv()
                pass_far(j).start()
                load_a(z_ref, s).start()

        @pl.when((s == PIECES - 1) & diag)
        def _():
            def go(q, carry):
                give_x(q).start()
                return carry
            lax.fori_loop(2, 2 * PIECES, go, 0)

        @pl.when(blk == 1)
        def _():
            @pl.when(diag)
            def _():
                pass_far(j).wait_recv()

            @pl.when(far)
            def _():
                pass_diag(j).wait_recv()
            load_a(z_ref, s).start()

        @pl.when((blk >= 2) & far)
        def _():
            give_x(s - 2 * PIECES).wait_recv()
            load_a(x_ref, s).start()

        load_a(a_ref, s).wait()

        @pl.when((s + 1 >= 2 * PIECES) & (s + 1 < steps) & diag)
        def _():
            load_a(a_ref, s + 1).start()

        load_b(b_ref, 0, s).wait()

        @pl.when(j == 0)
        def _():
            def body(n, carry):
                cs = pl.ds(pl.multiple_of(n * tile, tile), tile)
                acc[:, cs] = jnp.dot(av[slot], bv[slot, :, cs], preferred_element_type=jnp.float32)
                return carry
            lax.fori_loop(0, cols // tile, body, 0)

        @pl.when(j > 0)
        def _():
            def body(n, carry):
                cs = pl.ds(pl.multiple_of(n * tile, tile), tile)
                acc[:, cs] += jnp.dot(av[slot], bv[slot, :, cs], preferred_element_type=jnp.float32)
                return carry
            lax.fori_loop(0, cols // tile, body, 0)

        @pl.when((j == PIECES - 1) & (blk < 2))
        def _():
            store = pltpu.make_async_copy(acc, ps_ref.at[rows(base_of(blk), half)], p_sem)
            store.start()
            store.wait()
            give_c(blk).start()

        @pl.when((j == PIECES - 1) & (blk >= 2))
        def _():
            base = base_of(blk)
            give_c(blk - 2).wait_recv()
            n_out = cols // out_tile

            def part(n):
                return pl.ds(pl.multiple_of(n * out_tile, out_tile), out_tile)

            def fetch(n):
                at = lax.rem(n, 2)
                return pltpu.make_async_copy(pr_ref.at[rows(base, half), part(n)], prv.at[at], pr_sem.at[at])

            def put(n):
                at = lax.rem(n, 2)
                return pltpu.make_async_copy(ov.at[at], c_ref.at[rows(base, half), part(n)], o_sem.at[at])

            fetch(0).start()

            def finish(n, carry):
                at = lax.rem(n, 2)

                @pl.when(n + 1 < n_out)
                def _():
                    fetch(n + 1).start()
                fetch(n).wait()

                @pl.when(n >= 2)
                def _():
                    put(n - 2).wait()
                ov[at] = (acc[:, part(n)] + prv[at]).astype(ov.dtype)
                put(n).start()
                return carry
            lax.fori_loop(0, n_out, finish, 0)

            @pl.when(n_out >= 2)
            def _():
                put(n_out - 2).wait()
            put(n_out - 1).wait()
        return carry

    lax.fori_loop(0, steps, step, 0)

    def sent(src, sem):
        pltpu.make_async_remote_copy(src_ref=src, dst_ref=src, send_sem=sem, recv_sem=zf_recv.at[0],
                                     device_id=x_dev, device_id_type=MESH).wait_send()

    @pl.when(diag)
    def _():
        sent(t_ref, y_send)
        sent(z_ref.at[pl.ds(0, half - extra)], f_send)
        sent(a_ref, x_send)

    @pl.when(far)
    def _():
        sent(a_ref.at[pl.ds(0, half)], y_send)
        sent(z_ref.at[pl.ds(half, half)], f_send)
        sent(a_ref.at[pl.ds(half - extra, relay_rows)], x_send)

    def done_b(i, carry):
        give_b(i).wait_send()
        return carry
    lax.fori_loop(0, own, done_b, 0)
    give_c(0).wait_send()
    give_c(1).wait_send()


def solution(mesh, extra=EXTRA, tile=256, out_tile=768):
    grid_spec = P(("dp", "ri", "ro"), "co")

    def local_block(a_block, b_block):
        m, k = a_block.shape
        depth, n = b_block.shape
        half, kt = m // 2, k // PIECES
        bf16, f32 = jnp.bfloat16, jnp.float32
        hbm = pl.BlockSpec(memory_space=pl.ANY)
        dma = pltpu.SemaphoreType.DMA
        outs = pl.pallas_call(
            functools.partial(_kernel, extra, tile, out_tile),
            out_shape=[
                jax.ShapeDtypeStruct((m, n), bf16),
                jax.ShapeDtypeStruct((m, k), bf16),
                jax.ShapeDtypeStruct((m, k), bf16),
                jax.ShapeDtypeStruct((half + extra, k), bf16),
                jax.ShapeDtypeStruct((depth, n), bf16),
                jax.ShapeDtypeStruct((m, n), f32),
                jax.ShapeDtypeStruct((m, n), f32),
            ],
            in_specs=[hbm, hbm],
            out_specs=[hbm] * 7,
            scratch_shapes=[
                pltpu.VMEM((half, n), f32),
                pltpu.VMEM((2, half, kt), bf16),
                pltpu.VMEM((2, kt, n), bf16),
                pltpu.VMEM((2, half, out_tile), f32),
                pltpu.VMEM((2, half, out_tile), bf16),
                dma((PIECES,)), dma((PIECES,)), dma((PIECES,)), dma((2 * PIECES,)),
                dma((PIECES // 2,)), dma((2,)),
                dma, dma, dma, dma((PIECES // 2,)), dma((2,)),
                dma((2,)), dma((2,)), dma, dma((2,)), dma((2,)),
            ],
            compiler_params=pltpu.CompilerParams(
                collective_id=0, has_side_effects=True, vmem_limit_bytes=63_000_000),
        )(a_block, b_block)
        return outs[0]

    return jax.shard_map(local_block, mesh=mesh, in_specs=(grid_spec, grid_spec), out_specs=grid_spec, check_vma=False)
```

```python
import functools

import jax
import jax.numpy as jnp
from jax import lax
from jax.experimental import pallas as pl
from jax.experimental.pallas import tpu as pltpu
from jax.sharding import PartitionSpec as P

MESH = pl.DeviceIdType.MESH
PIECES = 16
EXTRA = 80
AHEAD = 8


def _kernel(extra, tile, out_tile, a_ref, b_ref, c_ref, z_ref, x_ref, t_ref, bs_ref, ps_ref, pr_ref,
            acc, zacc, av, bv, prv, ov, zf_recv, zg_recv, t_recv, x_recv, b_recv, c_recv,
            y_send, f_send, x_send, b_send, c_send, a_sem, b_sem, p_sem, pr_sem, o_sem):
    ri, co, ro = lax.axis_index("ri"), lax.axis_index("co"), lax.axis_index("ro")
    diag = ri == co
    far = ri != co
    x_dev, y_dev, sib = {"co": 1 - co}, {"ri": 1 - ri}, {"ro": 1 - ro}

    half = a_ref.shape[0] // 2
    quart = half // 2
    kt = a_ref.shape[1] // PIECES
    cols = b_ref.shape[1]
    own = PIECES // 2
    f = jnp.where(diag, 0, half)
    g = half - f

    def kcols(j):
        return pl.ds(pl.multiple_of(lax.rem(j + own * ro, PIECES) * kt, kt), kt)

    def rows(base, n):
        return pl.ds(pl.multiple_of(base, 8), n)

    def f_rows(h):
        return rows(jnp.where(diag, h, 3 - h) * quart, quart)

    def g_rows(h):
        return rows(jnp.where(diag, 3 - h, h) * quart, quart)

    def remote(src, dst, send, recv, dev):
        return pltpu.make_async_remote_copy(src_ref=src, dst_ref=dst, send_sem=send, recv_sem=recv,
                                            device_id=dev, device_id_type=MESH)

    def t_rows(h):
        return pl.ds(3 * quart, quart) if h == 0 else pl.ds(half - extra, quart + extra)

    def t_at(h):
        return pl.ds(quart + extra, quart) if h == 0 else pl.ds(0, quart + extra)

    def d_rows(h):
        return pl.ds(0, quart) if h == 0 else pl.ds(quart, quart - extra)

    def first_y(h, j):
        r = pl.ds(h * quart, quart)
        return remote(a_ref.at[r, kcols(j)], z_ref.at[r, kcols(j)], y_send, zf_recv.at[h, j], y_dev)

    def first_x(h, j):
        return remote(a_ref.at[t_rows(h), kcols(j)], t_ref.at[t_at(h), kcols(j)], x_send, t_recv.at[h, j], x_dev)

    def relay(h, j):
        return remote(t_ref.at[t_at(h), kcols(j)], z_ref.at[t_rows(h), kcols(j)], y_send, zf_recv.at[h, j], y_dev)

    def pass_diag(h, j):
        at = (d_rows(h), kcols(j))
        return remote(z_ref.at[at], z_ref.at[at], f_send, zg_recv.at[h, j], x_dev)

    def pass_far(h, j):
        at = (pl.ds((3 - h) * quart, quart), kcols(j))
        return remote(z_ref.at[at], z_ref.at[at], f_send, zg_recv.at[h, j], x_dev)

    def give_x(q):
        at = (rows(q // PIECES * half, half), kcols(lax.rem(q, PIECES)))
        return remote(a_ref.at[at], x_ref.at[at], x_send, x_recv.at[q], x_dev)

    def give_b(i):
        r = rows(i * kt, kt)
        return remote(b_ref.at[r], bs_ref.at[r], b_send.at[i], b_recv.at[i], sib)

    def give_c(q):
        r = (f_rows if q < 2 else g_rows)(q % 2)
        return remote(ps_ref.at[r], pr_ref.at[r], c_send.at[q], c_recv.at[q], y_dev)

    def load_a(src, r, j):
        slot = lax.rem(j, 2)
        n = quart if r.size == quart else half
        return pltpu.make_async_copy(src.at[r, kcols(j)], av.at[slot, pl.ds(0, n)], a_sem.at[slot])

    def start_b(j, fresh=False):
        slot = lax.rem(j, 2)

        @pl.when(j < own)
        def _():
            pltpu.make_async_copy(b_ref.at[rows(j * kt, kt)], bv.at[slot], b_sem.at[slot]).start()

        @pl.when(j >= own)
        def _():
            if fresh:
                give_b(j - own).wait_recv()
            pltpu.make_async_copy(bs_ref.at[rows((j - own) * kt, kt)], bv.at[slot], b_sem.at[slot]).start()

    def wait_b(j):
        slot = lax.rem(j, 2)
        pltpu.make_async_copy(b_ref.at[rows(0, kt)], bv.at[slot], b_sem.at[slot]).wait()

    def next_b(j, fresh=False, last=False):
        if last:
            @pl.when(j + 1 < PIECES)
            def _():
                start_b(j + 1)
        else:
            start_b(lax.rem(j + 1, PIECES), fresh)

    def multiply(total, n, j):
        slot = lax.rem(j, 2)

        def product(i):
            cs = pl.ds(pl.multiple_of(i * tile, tile), tile)
            return cs, jnp.dot(av[slot, :n], bv[slot, :, cs], preferred_element_type=jnp.float32)

        @pl.when(j == 0)
        def _():
            def body(i, carry):
                cs, part = product(i)
                total[:, cs] = part
                return carry
            lax.fori_loop(0, cols // tile, body, 0)

        @pl.when(j > 0)
        def _():
            def body(i, carry):
                cs, part = product(i)
                total[:, cs] += part
                return carry
            lax.fori_loop(0, cols // tile, body, 0)

    def store_total(r):
        store = pltpu.make_async_copy(zacc, ps_ref.at[r], p_sem)
        store.start()
        store.wait()

    n_out = cols // out_tile

    def finish(base, from_step):
        def part(n):
            return pl.ds(pl.multiple_of(n * out_tile, out_tile), out_tile)

        def fetch(n):
            at = lax.rem(n, 2)
            return pltpu.make_async_copy(pr_ref.at[rows(base, half), part(n)], prv.at[at], pr_sem.at[at])

        def put(n):
            at = lax.rem(n, 2)
            return pltpu.make_async_copy(ov.at[at], c_ref.at[rows(base, half), part(n)], o_sem.at[at])

        fetch(0).start()

        def body(n, carry):
            at = lax.rem(n, 2)

            @pl.when(n + 1 < n_out)
            def _():
                fetch(n + 1).start()
            fetch(n).wait()

            @pl.when(n >= 2)
            def _():
                put(n - 2).wait()
            for i in range(out_tile // tile):
                ts = pl.ds(i * tile, tile)
                cs = pl.ds(pl.multiple_of(n * out_tile + i * tile, tile), tile)
                total = acc[:, cs] + prv[at, :, ts]
                if from_step:
                    total += jnp.dot(av[(PIECES - 1) % 2], bv[(PIECES - 1) % 2, :, cs],
                                     preferred_element_type=jnp.float32)
                ov[at, :, ts] = total.astype(ov.dtype)
            put(n).start()
            return carry
        lax.fori_loop(0, n_out, body, 0)
        if n_out >= 2:
            put(n_out - 2).wait()
        put(n_out - 1).wait()

    barrier = pltpu.get_barrier_semaphore()
    for dev in (x_dev, y_dev, sib):
        pl.semaphore_signal(barrier, inc=1, device_id=dev, device_id_type=MESH)
    pl.semaphore_wait(barrier, 3)

    @pl.when(far)
    def _():
        for h in range(2):
            def go(j, carry):
                first_x(h, j).start()
                first_y(h, j).start()
                return carry
            lax.fori_loop(0, PIECES, go, 0)

    def go_x(q, carry):
        give_x(q).start()
        return carry

    @pl.when(diag)
    def _():
        lax.fori_loop(0, AHEAD, go_x, 0)

    def go_b(i, carry):
        give_b(i).start()
        return carry
    lax.fori_loop(0, own, go_b, 0)
    start_b(0)

    for h in range(2):
        def f_step(j, carry):
            next_b(j, fresh=h == 0)

            @pl.when(diag)
            def _():
                with jax.named_scope("wait_zf_diag"):
                    first_y(h, j).wait_recv()
                pass_diag(h, j).start()
                load_a(z_ref, f_rows(h), j).start()
                with jax.named_scope("wait_t"):
                    first_x(h, j).wait_recv()
                relay(h, j).start()

            @pl.when(far)
            def _():
                with jax.named_scope("wait_zf_far"):
                    relay(h, j).wait_recv()
                pass_far(h, j).start()
                load_a(z_ref, f_rows(h), j).start()
            load_a(z_ref, f_rows(h), j).wait()
            with jax.named_scope("wait_b"):
                wait_b(j)
            multiply(zacc, quart, j)
            return carry
        lax.fori_loop(0, PIECES, f_step, 0)

        if h == 1:
            @pl.when(diag)
            def _():
                lax.fori_loop(AHEAD, 2 * PIECES, go_x, 0)
        store_total(f_rows(h))
    give_c(0).start()
    give_c(1).start()

    def x_block(blk, base, diag_branch, last):
        src = a_ref if diag_branch else x_ref

        def x_step(j, carry):
            next_b(j, last=last)
            if diag_branch:
                load_a(src, rows(base, half), j).start()
            else:
                with jax.named_scope("wait_x"):
                    give_x(blk * PIECES + j).wait_recv()
                load_a(src, rows(base, half), j).start()
            load_a(src, rows(base, half), j).wait()
            wait_b(j)

            if last:
                @pl.when(j < PIECES - 1)
                def _():
                    multiply(acc, half, j)
            else:
                multiply(acc, half, j)
            return carry
        lax.fori_loop(0, PIECES, x_step, 0)

    @pl.when(diag)
    def _():
        with jax.named_scope("xg_diag"):
            x_block(0, g, True, False)

    for h in range(2):
        def g_step(j, carry):
            next_b(j)

            @pl.when(diag)
            def _():
                with jax.named_scope("wait_zg_diag"):
                    pass_far(h, j).wait_recv()

            @pl.when(far)
            def _():
                with jax.named_scope("wait_zg_far"):
                    pass_diag(h, j).wait_recv()
            load_a(z_ref, g_rows(h), j).start()
            load_a(z_ref, g_rows(h), j).wait()
            wait_b(j)
            multiply(zacc, quart, j)
            return carry
        lax.fori_loop(0, PIECES, g_step, 0)
        store_total(g_rows(h))
        give_c(2 + h).start()

    @pl.when(far)
    def _():
        with jax.named_scope("xg_far"):
            x_block(0, g, False, False)

    with jax.named_scope("wait_c_first"):
        give_c(0).wait_recv()
        give_c(1).wait_recv()
    with jax.named_scope("finish_first"):
        finish(g, False)

    @pl.when(diag)
    def _():
        x_block(1, f, True, True)

    @pl.when(far)
    def _():
        x_block(1, f, False, True)

    with jax.named_scope("wait_c_last"):
        give_c(2).wait_recv()
        give_c(3).wait_recv()
    with jax.named_scope("finish_last"):
        finish(f, True)

    def sent(src, sem):
        pltpu.make_async_remote_copy(src_ref=src, dst_ref=src, send_sem=sem, recv_sem=b_recv.at[0],
                                     device_id=x_dev, device_id_type=MESH).wait_send()

    @pl.when(diag)
    def _():
        sent(t_ref, y_send)
        sent(z_ref.at[pl.ds(0, half - extra)], f_send)
        sent(a_ref, x_send)

    @pl.when(far)
    def _():
        sent(a_ref.at[pl.ds(0, half)], y_send)
        sent(z_ref.at[pl.ds(half, half)], f_send)
        sent(t_ref, x_send)

    def done_b(i, carry):
        give_b(i).wait_send()
        return carry
    lax.fori_loop(0, own, done_b, 0)
    for q in range(4):
        give_c(q).wait_send()


def solution(mesh, extra=EXTRA, tile=256, out_tile=768):
    grid_spec = P(("dp", "ri", "ro"), "co")

    def local_block(a_block, b_block):
        m, k = a_block.shape
        depth, n = b_block.shape
        half, kt = m // 2, k // PIECES
        bf16, f32 = jnp.bfloat16, jnp.float32
        hbm = pl.BlockSpec(memory_space=pl.ANY)
        dma = pltpu.SemaphoreType.DMA
        outs = pl.pallas_call(
            functools.partial(_kernel, extra, tile, out_tile),
            out_shape=[
                jax.ShapeDtypeStruct((m, n), bf16),
                jax.ShapeDtypeStruct((m, k), bf16),
                jax.ShapeDtypeStruct((m, k), bf16),
                jax.ShapeDtypeStruct((half + extra, k), bf16),
                jax.ShapeDtypeStruct((depth, n), bf16),
                jax.ShapeDtypeStruct((m, n), f32),
                jax.ShapeDtypeStruct((m, n), f32),
            ],
            in_specs=[hbm, hbm],
            out_specs=[hbm] * 7,
            scratch_shapes=[
                pltpu.VMEM((half, n), f32),
                pltpu.VMEM((half // 2, n), f32),
                pltpu.VMEM((2, half, kt), bf16),
                pltpu.VMEM((2, kt, n), bf16),
                pltpu.VMEM((2, half, out_tile), f32),
                pltpu.VMEM((2, half, out_tile), bf16),
                dma((2, PIECES)), dma((2, PIECES)), dma((2, PIECES)), dma((2 * PIECES,)),
                dma((PIECES // 2,)), dma((4,)),
                dma, dma, dma, dma((PIECES // 2,)), dma((4,)),
                dma((2,)), dma((2,)), dma, dma((2,)), dma((2,)),
            ],
            compiler_params=pltpu.CompilerParams(
                collective_id=0, has_side_effects=True, vmem_limit_bytes=66_000_000),
        )(a_block, b_block)
        return outs[0]

    return jax.shard_map(local_block, mesh=mesh, in_specs=(grid_spec, grid_spec), out_specs=grid_spec, check_vma=False)
```

```python
import functools

import jax
import jax.numpy as jnp
from jax import lax
from jax.experimental import pallas as pl
from jax.experimental.pallas import tpu as pltpu
from jax.sharding import PartitionSpec as P

MESH = pl.DeviceIdType.MESH
PIECES = 16
EXTRA = 80
B_PARTS = 4


def _kernel(extra, tile, out_tile, a_ref, b_ref, c_ref, z_ref, x_ref, t_ref, bs_ref, ps_ref, pr_ref,
            acc, zacc, av, bv, prv, ov, zf_recv, zg_recv, t_recv, x_recv, b_recv, c_recv,
            y_send, f_send, x_send, b_send, c_send, a_sem, b_sem, p_sem, pr_sem, o_sem):
    ri, co, ro = lax.axis_index("ri"), lax.axis_index("co"), lax.axis_index("ro")
    diag = ri == co
    far = ri != co
    x_dev, y_dev, sib = {"co": 1 - co}, {"ri": 1 - ri}, {"ro": 1 - ro}

    half = a_ref.shape[0] // 2
    quart = half // 2
    kt = a_ref.shape[1] // PIECES
    cols = b_ref.shape[1]
    own = PIECES // 2
    f = jnp.where(diag, 0, half)
    g = half - f

    def kcols(j):
        return pl.ds(pl.multiple_of(lax.rem(j + own * ro, PIECES) * kt, kt), kt)

    def rows(base, n):
        return pl.ds(pl.multiple_of(base, 8), n)

    def f_rows(h):
        return rows(jnp.where(diag, h, 3 - h) * quart, quart)

    def g_rows(h):
        return rows(jnp.where(diag, 3 - h, h) * quart, quart)

    def remote(src, dst, send, recv, dev):
        return pltpu.make_async_remote_copy(src_ref=src, dst_ref=dst, send_sem=send, recv_sem=recv,
                                            device_id=dev, device_id_type=MESH)

    def t_rows(h):
        return pl.ds(3 * quart, quart) if h == 0 else pl.ds(half - extra, quart + extra)

    def t_at(h):
        return pl.ds(quart + extra, quart) if h == 0 else pl.ds(0, quart + extra)

    def d_rows(h):
        return pl.ds(0, quart) if h == 0 else pl.ds(quart, quart - extra)

    def first_y(h, j):
        r = pl.ds(h * quart, quart)
        return remote(a_ref.at[r, kcols(j)], z_ref.at[r, kcols(j)], y_send, zf_recv.at[h, j], y_dev)

    def first_x(h, j):
        return remote(a_ref.at[t_rows(h), kcols(j)], t_ref.at[t_at(h), kcols(j)], x_send, t_recv.at[h, j], x_dev)

    def relay(h, j):
        return remote(t_ref.at[t_at(h), kcols(j)], z_ref.at[t_rows(h), kcols(j)], y_send, zf_recv.at[h, j], y_dev)

    def pass_diag(h, j):
        at = (d_rows(h), kcols(j))
        return remote(z_ref.at[at], z_ref.at[at], f_send, zg_recv.at[h, j], x_dev)

    def pass_far(h, j):
        at = (pl.ds((3 - h) * quart, quart), kcols(j))
        return remote(z_ref.at[at], z_ref.at[at], f_send, zg_recv.at[h, j], x_dev)

    def give_x(q):
        at = (rows(q // PIECES * half, half), kcols(lax.rem(q, PIECES)))
        return remote(a_ref.at[at], x_ref.at[at], x_send, x_recv.at[q], x_dev)

    def give_b(i):
        r = rows(i * kt, kt)
        return remote(b_ref.at[r], bs_ref.at[r], b_send.at[i], b_recv.at[i], sib)

    def give_c(q):
        r = (f_rows if q < 2 else g_rows)(q % 2)
        return remote(ps_ref.at[r], pr_ref.at[r], c_send.at[q], c_recv.at[q], y_dev)

    def load_a(src, r, j):
        slot = lax.rem(j, 2)
        n = quart if r.size == quart else half
        return pltpu.make_async_copy(src.at[r, kcols(j)], av.at[slot, pl.ds(0, n)], a_sem.at[slot])

    def load_b(src, i, slot):
        n = kt // B_PARTS
        for p in range(B_PARTS):
            pltpu.make_async_copy(src.at[rows(i * kt + p * n, n)], bv.at[slot, pl.ds(p * n, n)], b_sem.at[slot]).start()

    def start_b(j, fresh=False):
        slot = lax.rem(j, 2)

        @pl.when(j < own)
        def _():
            load_b(b_ref, j, slot)

        @pl.when(j >= own)
        def _():
            if fresh:
                give_b(j - own).wait_recv()
            load_b(bs_ref, j - own, slot)

    def wait_b(j):
        slot = lax.rem(j, 2)
        with jax.named_scope("wait_b"):
            pltpu.make_async_copy(b_ref.at[rows(0, kt)], bv.at[slot], b_sem.at[slot]).wait()

    def next_b(j, fresh=False, last=False):
        if last:
            @pl.when(j + 1 < PIECES)
            def _():
                start_b(j + 1)
        else:
            start_b(lax.rem(j + 1, PIECES), fresh)

    def multiply(total, n, j):
        with jax.named_scope("mul"):
            multiply_in(total, n, j)

    def multiply_in(total, n, j):
        slot = lax.rem(j, 2)
        wide = out_tile // tile

        def products(i):
            for t in range(wide):
                cs = pl.ds(pl.multiple_of(i * out_tile + t * tile, tile), tile)
                yield cs, jnp.dot(av[slot, :n], bv[slot, :, cs], preferred_element_type=jnp.float32)

        @pl.when(j == 0)
        def _():
            def body(i, carry):
                for cs, part in products(i):
                    total[:, cs] = part
                return carry
            lax.fori_loop(0, cols // out_tile, body, 0)

        @pl.when(j > 0)
        def _():
            def body(i, carry):
                for cs, part in products(i):
                    total[:, cs] += part
                return carry
            lax.fori_loop(0, cols // out_tile, body, 0)

    def store_total(r):
        store = pltpu.make_async_copy(zacc, ps_ref.at[r], p_sem)
        store.start()
        store.wait()

    n_out = cols // out_tile

    def finish(base, from_step):
        def part(n):
            return pl.ds(pl.multiple_of(n * out_tile, out_tile), out_tile)

        def fetch(n):
            at = lax.rem(n, 2)
            return pltpu.make_async_copy(pr_ref.at[rows(base, half), part(n)], prv.at[at], pr_sem.at[at])

        def put(n):
            at = lax.rem(n, 2)
            return pltpu.make_async_copy(ov.at[at], c_ref.at[rows(base, half), part(n)], o_sem.at[at])

        fetch(0).start()

        def body(n, carry):
            at = lax.rem(n, 2)

            @pl.when(n + 1 < n_out)
            def _():
                fetch(n + 1).start()
            fetch(n).wait()

            @pl.when(n >= 2)
            def _():
                put(n - 2).wait()
            for i in range(out_tile // tile):
                ts = pl.ds(i * tile, tile)
                cs = pl.ds(pl.multiple_of(n * out_tile + i * tile, tile), tile)
                total = acc[:, cs] + prv[at, :, ts]
                if from_step:
                    total += jnp.dot(av[(PIECES - 1) % 2], bv[(PIECES - 1) % 2, :, cs],
                                     preferred_element_type=jnp.float32)
                ov[at, :, ts] = total.astype(ov.dtype)
            put(n).start()
            return carry
        lax.fori_loop(0, n_out, body, 0)
        if n_out >= 2:
            put(n_out - 2).wait()
        put(n_out - 1).wait()

    barrier = pltpu.get_barrier_semaphore()
    for dev in (x_dev, y_dev, sib):
        pl.semaphore_signal(barrier, inc=1, device_id=dev, device_id_type=MESH)
    pl.semaphore_wait(barrier, 3)

    @pl.when(far)
    def _():
        for h in range(2):
            def go(j, carry):
                first_x(h, j).start()
                first_y(h, j).start()
                if h == 0:
                    @pl.when(lax.rem(j, 2) == 0)
                    def _():
                        give_b(j // 2).start()
                return carry
            lax.fori_loop(0, PIECES, go, 0)

    def go_x(q, carry):
        give_x(q).start()
        return carry

    @pl.when(diag)
    def _():
        def go(i, carry):
            give_x(i).start()
            give_b(i).start()
            return carry
        lax.fori_loop(0, own, go, 0)
    start_b(0)

    for h in range(2):
        def f_step(j, carry):
            @pl.when(diag)
            def _():
                with jax.named_scope("wait_zf_diag"):
                    first_y(h, j).wait_recv()
                load_a(z_ref, f_rows(h), j).start()
                pass_diag(h, j).start()
                with jax.named_scope("wait_t"):
                    first_x(h, j).wait_recv()
                relay(h, j).start()

            @pl.when(far)
            def _():
                with jax.named_scope("wait_zf_far"):
                    relay(h, j).wait_recv()
                load_a(z_ref, f_rows(h), j).start()
                pass_far(h, j).start()
            next_b(j, fresh=h == 0)
            load_a(z_ref, f_rows(h), j).wait()
            wait_b(j)
            multiply(zacc, quart, j)
            return carry
        lax.fori_loop(0, PIECES, f_step, 0)

        if h == 1:
            @pl.when(diag)
            def _():
                lax.fori_loop(own, 2 * PIECES, go_x, 0)
        store_total(f_rows(h))
    give_c(0).start()
    give_c(1).start()

    def x_block(blk, base, diag_branch, last):
        src = a_ref if diag_branch else x_ref

        def bring(j):
            if not diag_branch:
                with jax.named_scope("wait_x"):
                    give_x(blk * PIECES + j).wait_recv()
            load_a(src, rows(base, half), j).start()

        late = last and not diag_branch
        ahead = PIECES - 1 if late else PIECES
        bring(0)

        def x_step(j, carry):
            if late:
                @pl.when(j == PIECES - 1)
                def _():
                    bring(j)

            @pl.when(j + 1 < ahead)
            def _():
                bring(j + 1)
            next_b(j, last=last)
            load_a(src, rows(base, half), j).wait()
            wait_b(j)

            if last:
                @pl.when(j < PIECES - 1)
                def _():
                    multiply(acc, half, j)
            else:
                multiply(acc, half, j)
            return carry
        lax.fori_loop(0, PIECES, x_step, 0)

    @pl.when(diag)
    def _():
        with jax.named_scope("xg_diag"):
            x_block(0, g, True, False)

    for h in range(2):
        def bring_z(j):
            @pl.when(diag)
            def _():
                with jax.named_scope("wait_zg_diag"):
                    pass_far(h, j).wait_recv()

            @pl.when(far)
            def _():
                with jax.named_scope("wait_zg_far"):
                    pass_diag(h, j).wait_recv()
            load_a(z_ref, g_rows(h), j).start()
        bring_z(0)

        def g_step(j, carry):
            @pl.when(j + 1 < PIECES)
            def _():
                bring_z(j + 1)
            next_b(j)
            load_a(z_ref, g_rows(h), j).wait()
            wait_b(j)
            multiply(zacc, quart, j)
            return carry
        lax.fori_loop(0, PIECES, g_step, 0)
        store_total(g_rows(h))
        give_c(2 + h).start()

    @pl.when(far)
    def _():
        with jax.named_scope("xg_far"):
            x_block(0, g, False, False)

    with jax.named_scope("wait_c_first"):
        give_c(0).wait_recv()
        give_c(1).wait_recv()
    with jax.named_scope("finish_first"):
        finish(g, False)

    @pl.when(diag)
    def _():
        x_block(1, f, True, True)

    @pl.when(far)
    def _():
        x_block(1, f, False, True)

    with jax.named_scope("wait_c_last"):
        give_c(2).wait_recv()
        give_c(3).wait_recv()
    with jax.named_scope("finish_last"):
        finish(f, True)

    def sent(src, sem):
        pltpu.make_async_remote_copy(src_ref=src, dst_ref=src, send_sem=sem, recv_sem=b_recv.at[0],
                                     device_id=x_dev, device_id_type=MESH).wait_send()

    @pl.when(diag)
    def _():
        sent(t_ref, y_send)
        sent(z_ref.at[pl.ds(0, half - extra)], f_send)
        sent(a_ref, x_send)

    @pl.when(far)
    def _():
        sent(a_ref.at[pl.ds(0, half)], y_send)
        sent(z_ref.at[pl.ds(half, half)], f_send)
        sent(t_ref, x_send)

    def done_b(i, carry):
        give_b(i).wait_send()
        return carry
    lax.fori_loop(0, own, done_b, 0)
    for q in range(4):
        give_c(q).wait_send()


def solution(mesh, extra=EXTRA, tile=256, out_tile=768):
    grid_spec = P(("dp", "ri", "ro"), "co")

    def local_block(a_block, b_block):
        m, k = a_block.shape
        depth, n = b_block.shape
        half, kt = m // 2, k // PIECES
        bf16, f32 = jnp.bfloat16, jnp.float32
        hbm = pl.BlockSpec(memory_space=pl.ANY)
        dma = pltpu.SemaphoreType.DMA
        outs = pl.pallas_call(
            functools.partial(_kernel, extra, tile, out_tile),
            out_shape=[
                jax.ShapeDtypeStruct((m, n), bf16),
                jax.ShapeDtypeStruct((m, k), bf16),
                jax.ShapeDtypeStruct((m, k), bf16),
                jax.ShapeDtypeStruct((half + extra, k), bf16),
                jax.ShapeDtypeStruct((depth, n), bf16),
                jax.ShapeDtypeStruct((m, n), f32),
                jax.ShapeDtypeStruct((m, n), f32),
            ],
            in_specs=[hbm, hbm],
            out_specs=[hbm] * 7,
            scratch_shapes=[
                pltpu.VMEM((half, n), f32),
                pltpu.VMEM((half // 2, n), f32),
                pltpu.VMEM((2, half, kt), bf16),
                pltpu.VMEM((2, kt, n), bf16),
                pltpu.VMEM((2, half, out_tile), f32),
                pltpu.VMEM((2, half, out_tile), bf16),
                dma((2, PIECES)), dma((2, PIECES)), dma((2, PIECES)), dma((2 * PIECES,)),
                dma((PIECES // 2,)), dma((4,)),
                dma, dma, dma, dma((PIECES // 2,)), dma((4,)),
                dma((2,)), dma((2,)), dma, dma((2,)), dma((2,)),
            ],
            compiler_params=pltpu.CompilerParams(
                collective_id=0, has_side_effects=True, vmem_limit_bytes=66_000_000),
        )(a_block, b_block)
        return outs[0]

    return jax.shard_map(local_block, mesh=mesh, in_specs=(grid_spec, grid_spec), out_specs=grid_spec, check_vma=False)
```

```python
import functools

import jax
import jax.numpy as jnp
from jax import lax
from jax.experimental import pallas as pl
from jax.experimental.pallas import tpu as pltpu
from jax.sharding import PartitionSpec as P

MESH = pl.DeviceIdType.MESH
PIECES = 16
EXTRA = 88
B_PARTS = 4


def _kernel(extra, tile, out_tile, a_ref, b_ref, c_ref, z_ref, x_ref, t_ref, bs_ref, ps_ref, pr_ref,
            acc, zacc, av, bv, prv, ov, zf_recv, zg_recv, t_recv, x_recv, b_recv, c_recv,
            y_send, f_send, x_send, b_send, c_send, a_sem, b_sem, p_sem, pr_sem, o_sem):
    ri, co, ro = lax.axis_index("ri"), lax.axis_index("co"), lax.axis_index("ro")
    diag = ri == co
    far = ri != co
    x_dev, y_dev, sib = {"co": 1 - co}, {"ri": 1 - ri}, {"ro": 1 - ro}

    half = a_ref.shape[0] // 2
    quart = half // 2
    kt = a_ref.shape[1] // PIECES
    cols = b_ref.shape[1]
    own = PIECES // 2
    f = jnp.where(diag, 0, half)
    g = half - f

    def kcols(j):
        return pl.ds(pl.multiple_of(lax.rem(j + own * ro, PIECES) * kt, kt), kt)

    def rows(base, n):
        return pl.ds(pl.multiple_of(base, 8), n)

    def f_rows(h):
        return rows(jnp.where(diag, h, 3 - h) * quart, quart)

    def g_rows(h):
        return rows(jnp.where(diag, 3 - h, h) * quart, quart)

    def remote(src, dst, send, recv, dev):
        return pltpu.make_async_remote_copy(src_ref=src, dst_ref=dst, send_sem=send, recv_sem=recv,
                                            device_id=dev, device_id_type=MESH)

    def t_rows(h):
        return pl.ds(3 * quart, quart) if h == 0 else pl.ds(half - extra, quart + extra)

    def t_at(h):
        return pl.ds(quart + extra, quart) if h == 0 else pl.ds(0, quart + extra)

    def d_rows(h):
        return pl.ds(0, quart) if h == 0 else pl.ds(quart, quart - extra)

    def first_y(h, j):
        r = pl.ds(h * quart, quart)
        return remote(a_ref.at[r, kcols(j)], z_ref.at[r, kcols(j)], y_send, zf_recv.at[h, j], y_dev)

    def first_x(h, j):
        return remote(a_ref.at[t_rows(h), kcols(j)], t_ref.at[t_at(h), kcols(j)], x_send, t_recv.at[h, j], x_dev)

    def relay(h, j):
        return remote(t_ref.at[t_at(h), kcols(j)], z_ref.at[t_rows(h), kcols(j)], y_send, zf_recv.at[h, j], y_dev)

    def pass_diag(h, j):
        at = (d_rows(h), kcols(j))
        return remote(z_ref.at[at], z_ref.at[at], f_send, zg_recv.at[h, j], x_dev)

    def pass_far(h, j):
        at = (pl.ds((3 - h) * quart, quart), kcols(j))
        return remote(z_ref.at[at], z_ref.at[at], f_send, zg_recv.at[h, j], x_dev)

    def give_x(q):
        at = (rows(q // PIECES * half, half), kcols(lax.rem(q, PIECES)))
        return remote(a_ref.at[at], x_ref.at[at], x_send, x_recv.at[q], x_dev)

    def give_last(h):
        at = (pl.ds((3 - h) * quart, quart), kcols(PIECES - 1))
        return remote(a_ref.at[at], x_ref.at[at], x_send, x_recv.at[2 * PIECES - 1 + h], x_dev)

    def give_b(i):
        r = rows(i * kt, kt)
        return remote(b_ref.at[r], bs_ref.at[r], b_send.at[i], b_recv.at[i], sib)

    def give_c(q):
        r = (f_rows if q < 2 else g_rows)(q % 2)
        return remote(ps_ref.at[r], pr_ref.at[r], c_send.at[q], c_recv.at[q], y_dev)

    def load_a(src, r, j):
        slot = lax.rem(j, 2)
        n = quart if r.size == quart else half
        return pltpu.make_async_copy(src.at[r, kcols(j)], av.at[slot, pl.ds(0, n)], a_sem.at[slot])

    def load_b(src, i, slot):
        n = kt // B_PARTS
        for p in range(B_PARTS):
            pltpu.make_async_copy(src.at[rows(i * kt + p * n, n)], bv.at[slot, pl.ds(p * n, n)], b_sem.at[slot]).start()

    def start_b(j, fresh=False):
        slot = lax.rem(j, 2)

        @pl.when(j < own)
        def _():
            load_b(b_ref, j, slot)

        @pl.when(j >= own)
        def _():
            if fresh:
                give_b(j - own).wait_recv()
            load_b(bs_ref, j - own, slot)

    def wait_b(j):
        slot = lax.rem(j, 2)
        with jax.named_scope("wait_b"):
            pltpu.make_async_copy(b_ref.at[rows(0, kt)], bv.at[slot], b_sem.at[slot]).wait()

    def next_b(j, fresh=False):
        start_b(lax.rem(j + 1, PIECES), fresh)

    def multiply(total, n, j):
        with jax.named_scope("mul"):
            multiply_in(total, n, j)

    def multiply_in(total, n, j):
        slot = lax.rem(j, 2)
        wide = out_tile // tile

        def products(i):
            for t in range(wide):
                cs = pl.ds(pl.multiple_of(i * out_tile + t * tile, tile), tile)
                yield cs, jnp.dot(av[slot, :n], bv[slot, :, cs], preferred_element_type=jnp.float32)

        @pl.when(j == 0)
        def _():
            def body(i, carry):
                for cs, part in products(i):
                    total[:, cs] = part
                return carry
            lax.fori_loop(0, cols // out_tile, body, 0)

        @pl.when(j > 0)
        def _():
            def body(i, carry):
                for cs, part in products(i):
                    total[:, cs] += part
                return carry
            lax.fori_loop(0, cols // out_tile, body, 0)

    def store_total(r):
        store = pltpu.make_async_copy(zacc, ps_ref.at[r], p_sem)
        store.start()
        store.wait()

    n_out = cols // out_tile

    def finish(r, at_row, n_rows, piece_row=None):
        tall = pl.ds(0, n_rows)

        def part(n):
            return pl.ds(pl.multiple_of(n * out_tile, out_tile), out_tile)

        def fetch(n):
            at = lax.rem(n, 2)
            return pltpu.make_async_copy(pr_ref.at[r, part(n)], prv.at[at, tall], pr_sem.at[at])

        def put(n):
            at = lax.rem(n, 2)
            return pltpu.make_async_copy(ov.at[at, tall], c_ref.at[r, part(n)], o_sem.at[at])

        fetch(0).start()

        def body(n, carry):
            at = lax.rem(n, 2)

            @pl.when(n + 1 < n_out)
            def _():
                fetch(n + 1).start()
            fetch(n).wait()

            @pl.when(n >= 2)
            def _():
                put(n - 2).wait()
            for i in range(out_tile // tile):
                ts = pl.ds(i * tile, tile)
                cs = pl.ds(pl.multiple_of(n * out_tile + i * tile, tile), tile)
                total = acc[pl.ds(at_row, n_rows), cs] + prv[at, :n_rows, ts]
                if piece_row is not None:
                    slot = (PIECES - 1) % 2
                    total += jnp.dot(av[slot, piece_row:piece_row + n_rows], bv[slot, :, cs],
                                     preferred_element_type=jnp.float32)
                ov[at, :n_rows, ts] = total.astype(ov.dtype)
            put(n).start()
            return carry
        lax.fori_loop(0, n_out, body, 0)
        if n_out >= 2:
            put(n_out - 2).wait()
        put(n_out - 1).wait()

    def finish_last():
        wait_b(PIECES - 1)
        slot = (PIECES - 1) % 2
        for h in range(2):
            def bring(src):
                return pltpu.make_async_copy(src.at[f_rows(h), kcols(PIECES - 1)],
                                             av.at[slot, pl.ds(h * quart, quart)], a_sem.at[slot])

            @pl.when(diag)
            def _():
                bring(a_ref).start()

            @pl.when(far)
            def _():
                give_last(h).wait_recv()
                bring(x_ref).start()
            give_c(2 + h).wait_recv()
            bring(a_ref).wait()
            at_row = pl.multiple_of(jnp.where(diag, h, 1 - h) * quart, 8)
            finish(f_rows(h), at_row, quart, h * quart)

    barrier = pltpu.get_barrier_semaphore()
    for dev in (x_dev, y_dev, sib):
        pl.semaphore_signal(barrier, inc=1, device_id=dev, device_id_type=MESH)
    pl.semaphore_wait(barrier, 3)

    @pl.when(far)
    def _():
        for h in range(2):
            def go(j, carry):
                first_x(h, j).start()
                first_y(h, j).start()
                if h == 0:
                    @pl.when(lax.rem(j, 2) == 0)
                    def _():
                        give_b(j // 2).start()
                return carry
            lax.fori_loop(0, PIECES, go, 0)

    def go_x(q, carry):
        give_x(q).start()
        return carry

    @pl.when(diag)
    def _():
        def go(i, carry):
            give_x(i).start()
            give_b(i).start()
            return carry
        lax.fori_loop(0, own, go, 0)
    start_b(0)

    for h in range(2):
        def f_step(j, carry):
            @pl.when(diag)
            def _():
                with jax.named_scope("wait_zf_diag"):
                    first_y(h, j).wait_recv()
                load_a(z_ref, f_rows(h), j).start()
                pass_diag(h, j).start()
                with jax.named_scope("wait_t"):
                    first_x(h, j).wait_recv()
                relay(h, j).start()

            @pl.when(far)
            def _():
                with jax.named_scope("wait_zf_far"):
                    relay(h, j).wait_recv()
                load_a(z_ref, f_rows(h), j).start()
                pass_far(h, j).start()
            next_b(j, fresh=h == 0)
            load_a(z_ref, f_rows(h), j).wait()
            wait_b(j)
            multiply(zacc, quart, j)
            return carry
        lax.fori_loop(0, PIECES, f_step, 0)

        if h == 1:
            @pl.when(diag)
            def _():
                lax.fori_loop(own, 2 * PIECES - 1, go_x, 0)
                give_last(0).start()
                give_last(1).start()
        store_total(f_rows(h))
    give_c(0).start()
    give_c(1).start()

    def x_block(blk, base, diag_branch, last):
        src = a_ref if diag_branch else x_ref

        def bring(j):
            if not diag_branch:
                with jax.named_scope("wait_x"):
                    give_x(blk * PIECES + j).wait_recv()
            load_a(src, rows(base, half), j).start()

        count = PIECES - 1 if last else PIECES
        bring(0)

        def x_step(j, carry):
            @pl.when(j + 1 < count)
            def _():
                bring(j + 1)
            next_b(j)
            load_a(src, rows(base, half), j).wait()
            wait_b(j)
            multiply(acc, half, j)
            return carry
        lax.fori_loop(0, count, x_step, 0)

    @pl.when(diag)
    def _():
        with jax.named_scope("xg_diag"):
            x_block(0, g, True, False)

    for h in range(2):
        def bring_z(j):
            @pl.when(diag)
            def _():
                with jax.named_scope("wait_zg_diag"):
                    pass_far(h, j).wait_recv()

            @pl.when(far)
            def _():
                with jax.named_scope("wait_zg_far"):
                    pass_diag(h, j).wait_recv()
            load_a(z_ref, g_rows(h), j).start()
        bring_z(0)

        def g_step(j, carry):
            @pl.when(j + 1 < PIECES)
            def _():
                bring_z(j + 1)
            next_b(j)
            load_a(z_ref, g_rows(h), j).wait()
            wait_b(j)
            multiply(zacc, quart, j)
            return carry
        lax.fori_loop(0, PIECES, g_step, 0)
        store_total(g_rows(h))
        give_c(2 + h).start()

    @pl.when(far)
    def _():
        with jax.named_scope("xg_far"):
            x_block(0, g, False, False)

    with jax.named_scope("wait_c_first"):
        give_c(0).wait_recv()
        give_c(1).wait_recv()
    with jax.named_scope("finish_first"):
        finish(rows(g, half), 0, half)

    @pl.when(diag)
    def _():
        x_block(1, f, True, True)

    @pl.when(far)
    def _():
        x_block(1, f, False, True)

    finish_last()

    def sent(src, sem):
        pltpu.make_async_remote_copy(src_ref=src, dst_ref=src, send_sem=sem, recv_sem=b_recv.at[0],
                                     device_id=x_dev, device_id_type=MESH).wait_send()

    @pl.when(diag)
    def _():
        sent(t_ref, y_send)
        sent(z_ref.at[pl.ds(0, half - extra)], f_send)
        sent(a_ref, x_send)

    @pl.when(far)
    def _():
        sent(a_ref.at[pl.ds(0, half)], y_send)
        sent(z_ref.at[pl.ds(half, half)], f_send)
        sent(t_ref, x_send)

    def done_b(i, carry):
        give_b(i).wait_send()
        return carry
    lax.fori_loop(0, own, done_b, 0)
    for q in range(4):
        give_c(q).wait_send()


def solution(mesh, extra=EXTRA, tile=256, out_tile=768):
    grid_spec = P(("dp", "ri", "ro"), "co")

    def local_block(a_block, b_block):
        m, k = a_block.shape
        depth, n = b_block.shape
        half, kt = m // 2, k // PIECES
        bf16, f32 = jnp.bfloat16, jnp.float32
        hbm = pl.BlockSpec(memory_space=pl.ANY)
        dma = pltpu.SemaphoreType.DMA
        outs = pl.pallas_call(
            functools.partial(_kernel, extra, tile, out_tile),
            out_shape=[
                jax.ShapeDtypeStruct((m, n), bf16),
                jax.ShapeDtypeStruct((m, k), bf16),
                jax.ShapeDtypeStruct((m, k), bf16),
                jax.ShapeDtypeStruct((half + extra, k), bf16),
                jax.ShapeDtypeStruct((depth, n), bf16),
                jax.ShapeDtypeStruct((m, n), f32),
                jax.ShapeDtypeStruct((m, n), f32),
            ],
            in_specs=[hbm, hbm],
            out_specs=[hbm] * 7,
            scratch_shapes=[
                pltpu.VMEM((half, n), f32),
                pltpu.VMEM((half // 2, n), f32),
                pltpu.VMEM((2, half, kt), bf16),
                pltpu.VMEM((2, kt, n), bf16),
                pltpu.VMEM((2, half, out_tile), f32),
                pltpu.VMEM((2, half, out_tile), bf16),
                dma((2, PIECES)), dma((2, PIECES)), dma((2, PIECES)), dma((2 * PIECES + 1,)),
                dma((PIECES // 2,)), dma((4,)),
                dma, dma, dma, dma((PIECES // 2,)), dma((4,)),
                dma((2,)), dma((2,)), dma, dma((2,)), dma((2,)),
            ],
            compiler_params=pltpu.CompilerParams(
                collective_id=0, has_side_effects=True, vmem_limit_bytes=66_000_000),
        )(a_block, b_block)
        return outs[0]

    return jax.shard_map(local_block, mesh=mesh, in_specs=(grid_spec, grid_spec), out_specs=grid_spec, check_vma=False)
```
